32 devices in a mesh: row: 4 (over y, x), col: 4 (over z), batch: 2 (over core).
Axes of the slice: x: 2, y: 2, z: 4, core: 2. Of those that a mesh axis runs over, the one named last changes fastest.
Arguments:
- item_ids: int32 [4, 4, 2048], P('batch', 'col', 'row'), parts along dimension 0, may hold values from 0 to 511
- pad_masks: int32 [4, 4, 2048], P('batch', 'col', 'row'), parts along dimension 0, may hold values from 0 to 1
- lengths: int32 [4], P('batch'), parts along dimension 0, may hold values from 7168 to 8192
- item_table: bfloat16 [512, 1024], replicated, may hold values from -5 to 5
- w_gate: bfloat16 [1024, 1024], replicated, may hold values from -0.1875 to 0.1875
- w_in: bfloat16 [1024, 1280], replicated, may hold values from -0.1875 to 0.1875
- w_dt: bfloat16 [1024, 8], replicated, may hold values from -0.1875 to 0.1875
- conv_taps: float32 [4, 1280], replicated, may hold values from -3 to 3
- dt_bias: float32 [8], replicated, may hold values from -2 to 1
- decay_rates: float32 [8], replicated, may hold values from 1.2207031e-05 to 0.05
- norm_gain: float32 [1024], replicated, may hold values from 0.1 to 1.9
- w_out: bfloat16 [1024, 1024], replicated, may hold values from -0.1875 to 0.1875
Outputs:
- result: bfloat16 [4, 4, 2048, 1024], P('batch', 'col', 'row'), parts along dimension 0
The draws below stay inside these ranges and needn't reach their ends.
There are 2 independent parts, one for each index of `batch`. The reference program is written for one: setup_inputs(seed, part) draws one part's arguments, and reference() takes and returns one part's arrays. A program takes and returns all parts, laid end to end along the dimension named above; an argument that names none is the same for every part. Nothing has to cross between parts.
Inputs may be any that keep to these rules, and one draw needn't show every extreme that they name: `lengths`: every history keeps at least its first 7168 positions before padding.
All inputs are finite; a program needn't handle non-finite values.
Results may differ from the reference program's by a relative error of at most 0.0093.
Values may be sent and summed in bfloat16 or wider, within the bound.
A program may use at most 128 MiB of HBM per device.

```python
import math
import jax
import jax.numpy as jnp
import numpy as np
from jax import lax

D = 1024
H = 8
NS = 128
KW = 4
STRETCH = 128
ITEMS = 512
SEQS = 2
TOK_DEV = 512
DI = 1024
BLOCKS = 4
BLOCK_LEN = 2048
LENGTH = 8192


def draw_pad_masks(key, part):
    level_key = jax.random.fold_in(key, 17)
    entry_key = jax.random.fold_in(key, 29)
    spans = BLOCK_LEN // TOK_DEV
    levels = jax.random.randint(level_key, (SEQS, BLOCKS, spans, 1), 1, 5, dtype=jnp.int32)
    entries = jax.random.randint(entry_key, (SEQS, BLOCKS, spans, TOK_DEV), 0, 4, dtype=jnp.int32)
    kept = (entries < levels).astype(jnp.int32)
    return kept.reshape(SEQS, BLOCKS, BLOCK_LEN)


def place_ends(values, key, least, largest):
    dims = values.shape
    spot = [jax.random.randint(jax.random.fold_in(key, axis), (), 0, dims[axis]) for axis in range(len(dims))]
    values = values.at[tuple(spot)].set(least)
    longest = dims.index(max(dims))
    spot[longest] = (spot[longest] + 1) % dims[longest]
    return values.at[tuple(spot)].set(largest)


def cumulative_ranks(number_of, skew):
    loads = [(1 << 20) // math.isqrt(grade ** skew) + 1 for grade in range(1, number_of + 1)]
    deviation = 1 + sum(loads) // (1 << 30)
    return np.cumsum(np.array([max(1, weight // deviation) for weight in loads]))


def ranked_ids(rng, shape, count, skew):
    listing = cumulative_ranks(count, skew)
    lot = jax.random.randint(jax.random.fold_in(rng, 1), shape, 0, int(listing[count - 1]))
    rank = jnp.searchsorted(jnp.asarray(listing, jnp.int32), lot, side="right")
    return jax.random.permutation(jax.random.fold_in(rng, 2), count)[rank].astype(jnp.int32)


def gaussian(rng, extent, width, bound, kind=jnp.bfloat16):
    array = jax.random.normal(rng, extent, jnp.float32) * width
    return jnp.minimum(jnp.maximum(array, -bound), bound).astype(kind)


def setup_inputs(seed: int = 0, part: int = 0) -> dict:
    key_list = jax.random.split(jax.random.key(seed), 13)
    part_keys = jax.random.split(jax.random.fold_in(key_list[12], part), 13)
    return {
        "item_ids": place_ends(ranked_ids(part_keys[0], (SEQS, BLOCKS, BLOCK_LEN), ITEMS, 2), jax.random.fold_in(part_keys[0], 3), 0, ITEMS - 1).astype(jnp.int32),
        "pad_masks": draw_pad_masks(jax.random.fold_in(jax.random.fold_in(key_list[12], part), 71), part),
        "lengths": jax.random.randint(part_keys[2], (SEQS,), LENGTH - BLOCK_LEN // 2, LENGTH + 1).astype(jnp.int32),
        "item_table": gaussian(key_list[3], (ITEMS, D), 1.0, 5.0),
        "w_gate": gaussian(key_list[4], (D, DI), D ** -0.5, 0.1875),
        "w_in": gaussian(key_list[5], (D, DI + 2 * NS), D ** -0.5, 0.1875),
        "w_dt": gaussian(key_list[6], (D, H), D ** -0.5, 0.1875),
        "conv_taps": gaussian(key_list[7], (KW, DI + 2 * NS), 0.5, 3.0, jnp.float32),
        "dt_bias": jnp.clip(jax.random.uniform(key_list[8], (H,), jnp.float32, -2.0, 1.0), -2.0, 1.0),
        "decay_rates": jnp.clip(jnp.exp(jax.random.uniform(key_list[9], (H,), jnp.float32, math.log(1.220703143189894e-05), math.log(0.05))), 1.220703143189894e-05, 0.05),
        "norm_gain": jnp.clip(1.0 + 0.18 * jax.random.normal(key_list[10], (DI,), jnp.float32), 0.1, 1.9),
        "w_out": gaussian(key_list[11], (DI, D), DI ** -0.5, 0.1875),
    }


def rounded(value):
    return lax.optimization_barrier(value.astype(jnp.bfloat16)).astype(jnp.float32)

def reference(item_ids, pad_masks, lengths, item_table, w_gate, w_in, w_dt, conv_taps, dt_bias, decay_rates, norm_gain, w_out):
    users = item_ids.shape[0]
    events = item_ids.shape[1] * item_ids.shape[2]
    stretch_count = events // STRETCH
    full_width = w_in.shape[1]
    inner_width = w_gate.shape[1]
    head_count = decay_rates.shape[0]
    head_size = inner_width // head_count
    state_width = (full_width - inner_width) // 2
    kernel = conv_taps.shape[0]
    item_stretches = item_ids.reshape(users, stretch_count, STRETCH).transpose(1, 0, 2)
    mask_stretches = pad_masks.reshape(users, stretch_count, STRETCH).transpose(1, 0, 2)
    starts = jnp.arange(stretch_count, dtype=jnp.int32) * STRETCH
    within = jnp.arange(STRETCH, dtype=jnp.int32)
    causal = within[:, None] >= within[None, :]

    def advance(carried, inputs):
        state_now, before = carried
        item_rows, mask_rows, start = inputs
        embedded = jnp.take(item_table, item_rows, axis=0).reshape(users * STRETCH, -1)
        projected = jnp.dot(embedded, w_in, preferred_element_type=jnp.float32).astype(jnp.bfloat16).reshape(users, STRETCH, full_width)
        gate_rows = rounded(jnp.dot(embedded, w_gate, preferred_element_type=jnp.float32)).reshape(users, STRETCH, inner_width)
        step_raw = jnp.dot(embedded, w_dt, preferred_element_type=jnp.float32).reshape(users, STRETCH, head_count)
        joined = lax.optimization_barrier(jnp.concatenate([before, projected], axis=1)).astype(jnp.float32)
        convolved = joined[:, 0:STRETCH, :] * conv_taps[0]
        for offset in range(1, kernel):
            convolved = convolved + joined[:, offset:offset + STRETCH, :] * conv_taps[offset]
        signal = rounded(jax.nn.silu(convolved[..., :inner_width]))
        inward = rounded(convolved[..., inner_width:inner_width + state_width])
        outward = rounded(convolved[..., inner_width + state_width:])
        position = start + within
        usable = jnp.logical_and(position[None, :] < lengths[:, None], mask_rows > 0).astype(jnp.float32)
        step_size = usable[..., None] * jax.nn.softplus(step_raw + dt_bias)
        log_decay = jnp.cumsum(step_size * decay_rates, axis=1)
        log_heads = log_decay.transpose(0, 2, 1)
        size_heads = step_size.transpose(0, 2, 1)
        scores = jnp.einsum('sqn,sun->squ', outward, inward)
        log_gap = log_heads[:, :, :, None] - log_heads[:, :, None, :]
        decays = jnp.where(causal, jnp.exp(-jnp.where(causal, log_gap, 0.0)), 0.0)
        weights = rounded(scores[:, None] * decays * size_heads[:, :, None, :])
        signal_heads = signal.reshape(users, STRETCH, head_count, head_size)
        local_out = jnp.einsum('shqu,suhp->sqhp', weights, signal_heads)
        entering = rounded(state_now)
        carried_out = jnp.einsum('sqn,shpn->sqhp', outward, entering) * jnp.exp(-log_decay)[..., None]
        mixture = (local_out + carried_out).reshape(users, STRETCH, inner_width)
        gated_rows = mixture * jax.nn.silu(gate_rows)
        normed = (gated_rows * lax.rsqrt(lax.optimization_barrier(jnp.mean(gated_rows * gated_rows, axis=-1, keepdims=True)) + 1.0) * norm_gain).astype(jnp.bfloat16)
        result = jnp.dot(normed.reshape(users * STRETCH, inner_width), w_out, preferred_element_type=jnp.float32).reshape(users, STRETCH, -1)
        result = (result * usable[..., None]).astype(jnp.bfloat16)
        tail_weight = jnp.exp(log_heads - log_heads[:, :, -1:]) * size_heads
        scaled_in = rounded(inward[:, None, :, :] * tail_weight[..., None])
        stretch_state = jnp.einsum('shun,suhp->shpn', scaled_in, signal_heads)
        new_state = jnp.exp(-log_heads[:, :, -1])[..., None, None] * state_now + stretch_state
        return ((new_state, projected[:, STRETCH - (kernel - 1):, :]), result)
    initial = (jnp.zeros((users, head_count, head_size, state_width), jnp.float32), jnp.zeros((users, kernel - 1, full_width), jnp.bfloat16))
    _, results = lax.scan(advance, initial, (item_stretches, mask_stretches, starts))
    return results.transpose(1, 0, 2, 3).reshape(item_ids.shape + (item_table.shape[1],))
```

```python
import functools

import jax
import jax.numpy as jnp
from jax import lax
from jax.experimental import pallas as pl
from jax.experimental.pallas import tpu as pltpu
from jax.sharding import PartitionSpec as P

STRETCH = 128
LANES = 128
HALO = 16
MESH = pl.DeviceIdType.MESH
F32 = jnp.float32
BF16 = jnp.bfloat16


def silu(v):
    return 0.5 * v * (1.0 + jnp.tanh(0.5 * v))


def local_kernel(
    counts,
    meta_ref,
    tin_ref,
    tgate_ref,
    tdt_ref,
    taps_ref,
    bias_ref,
    rates_ref,
    y_ref,
    gate_ref,
    out_ref,
    ef_ref,
    state_ref,
    log_ref,
    pbuf,
    scaled,
    run,
    cum,
):
    stretch_count, head_count, head_size, state_width, pieces = counts
    inner = head_count * head_size
    place = lax.rem(pl.program_id(0), stretch_count)

    @pl.when(place == 0)
    def _():
        run[...] = jnp.zeros_like(run)
        cum[...] = jnp.zeros_like(cum)

    meta = jnp.transpose(meta_ref[0])
    ids = meta[: HALO + STRETCH, 0:1].astype(jnp.int32)
    usable = meta[:STRETCH, 1:2]
    items = tin_ref.shape[0]
    hot = (ids == lax.broadcasted_iota(jnp.int32, (HALO + STRETCH, items), 1)).astype(F32).astype(BF16)
    pbuf[...] = jnp.dot(hot, tin_ref[...], preferred_element_type=F32)
    now = hot[HALO:]
    gate_ref[...] = jnp.dot(now, tgate_ref[...], preferred_element_type=F32).astype(BF16)
    parts = jnp.dot(now, tdt_ref[...], preferred_element_type=F32)
    raw = (
        parts
        + pltpu.roll(parts, LANES - head_count, 1)
        + pltpu.roll(parts, LANES - 2 * head_count, 1)
    )
    raw = raw + bias_ref[...]
    step = usable * (jnp.maximum(raw, 0.0) + jnp.log1p(jnp.exp(-jnp.abs(raw))))
    rows = lax.broadcasted_iota(jnp.int32, (STRETCH, STRETCH), 0)
    cols = lax.broadcasted_iota(jnp.int32, (STRETCH, STRETCH), 1)
    causal = rows >= cols
    logs = jnp.dot(
        jnp.where(causal, 1.0, 0.0).astype(F32),
        step * rates_ref[...],
        precision=lax.Precision.HIGHEST,
        preferred_element_type=F32,
    )
    total = logs[STRETCH - 1 :, :]
    logs_t = jnp.transpose(logs)
    step_t = jnp.transpose(step)
    kernel = taps_ref.shape[0]
    conv = None
    for k in range(kernel):
        start = HALO - (kernel - 1) + k
        term = pbuf[start : start + STRETCH, :] * taps_ref[k : k + 1, :]
        conv = term if conv is None else conv + term
    signal = silu(conv[:, :inner]).astype(BF16)
    inward = conv[:, inner : inner + state_width].astype(BF16)
    outward = conv[:, inner + state_width :].astype(BF16)
    out_ref[...] = outward
    scores = lax.dot_general(
        outward, inward, (((1,), (1,)), ((), ())), preferred_element_type=F32
    )
    scores = jnp.where(causal, scores, 0.0)
    tail = jnp.exp(logs - total) * step
    fade = jnp.exp(-logs)
    held = jnp.dot(outward, run[...].astype(BF16), preferred_element_type=F32)
    for h in range(head_count):
        span = slice(h * head_size, (h + 1) * head_size)
        gap = jnp.minimum(logs_t[h : h + 1, :] - logs[:, h : h + 1], 0.0)
        weights = (jnp.exp(gap) * (scores * step_t[h : h + 1, :])).astype(BF16)
        near = jnp.dot(weights, signal[:, span], preferred_element_type=F32)
        y_ref[:, span] = near + held[:, span] * fade[:, h : h + 1]
        scaled[:, span] = (signal[:, span].astype(F32) * tail[:, h : h + 1]).astype(BF16)
    added = lax.dot_general(
        inward, scaled[...], (((0,), (0,)), ((), ())), preferred_element_type=F32
    )
    shrink = jnp.exp(-total)
    for h in range(head_count):
        span = slice(h * head_size, (h + 1) * head_size)
        run[:, span] = run[:, span] * shrink[:, h : h + 1] + added[:, span]
    before = cum[0:1, :]
    lane = lax.broadcasted_iota(jnp.int32, (STRETCH, LANES), 1)
    ef_ref[...] = jnp.where(lane == LANES - 1, usable, jnp.exp(-(logs + before)))
    after = before + total
    cum[...] = jnp.broadcast_to(after, cum.shape)

    @pl.when(place == stretch_count - 1)
    def _():
        width = inner // pieces
        for q in range(pieces):
            state_ref[q, 0] = run[:, q * width : (q + 1) * width].astype(BF16)
            for j in range(width // head_size):
                h = q * (width // head_size) + j
                log_ref[q, 0, :, j * head_size : (j + 1) * head_size] = jnp.broadcast_to(
                    after[:, h : h + 1], (8, head_size)
                )


def chain_kernel(
    rows,
    cols,
    state_ref,
    log_ref,
    enter_ref,
    rin,
    lin,
    before,
    fades,
    pin,
    psend,
    esend,
    s1,
    r1,
    sl,
    rl,
    s2,
    r2,
    s3,
    r3,
):
    users = state_ref.shape[1]
    r, c = lax.axis_index("row"), lax.axis_index("col")
    barrier = pltpu.get_barrier_semaphore()
    for d in range(1, rows):
        pl.semaphore_signal(
            barrier, inc=1, device_id={"row": lax.rem(r + d, rows)}, device_id_type=MESH
        )

    @pl.when(c > 0)
    def _():
        pl.semaphore_signal(barrier, inc=1, device_id={"col": c - 1}, device_id_type=MESH)

    @pl.when(c < cols - 1)
    def _():
        pl.semaphore_signal(barrier, inc=1, device_id={"col": c + 1}, device_id_type=MESH)

    peers = rows - 1 + jnp.where(c > 0, 1, 0) + jnp.where(c < cols - 1, 1, 0)
    pl.semaphore_wait(barrier, peers)

    first = []
    for d in range(1, rows):
        q = lax.rem(r + d, rows)
        for source, target, send, recv in (
            (log_ref, lin, sl, rl),
            (state_ref, rin, s1, r1),
        ):
            copy = pltpu.make_async_remote_copy(
                src_ref=source.at[q],
                dst_ref=target.at[r],
                send_sem=send.at[d],
                recv_sem=recv.at[d],
                device_id={"row": q},
                device_id_type=MESH,
            )
            copy.start()
            first.append(copy)
    rin[r] = state_ref[r]
    lin[r] = log_ref[r]
    for copy in first:
        copy.wait()

    for u in range(users):
        carried = jnp.zeros(pin.shape[1:], F32)
        fade = jnp.ones((1, pin.shape[2]), F32)
        for m in range(rows):
            before[m, u] = carried
            fades[m, u] = jnp.broadcast_to(fade, fades.shape[2:])
            here = jnp.exp(-lin[m, u, 0:1, :])
            carried = here * carried + rin[m, u].astype(F32)
            fade = fade * here
        before[rows, u] = carried
        fades[rows, u] = jnp.broadcast_to(fade, fades.shape[2:])

    @pl.when(c == 0)
    def _():
        pin[...] = jnp.zeros_like(pin)

    second = []
    third = []
    for u in range(users):
        copy = pltpu.make_async_remote_copy(
            src_ref=psend.at[u],
            dst_ref=pin.at[u],
            send_sem=s2.at[u],
            recv_sem=r2.at[u],
            device_id={"col": lax.rem(c + 1, cols)},
            device_id_type=MESH,
        )
        second.append(copy)

        @pl.when(c > 0)
        def _(copy=copy):
            copy.wait_recv()

        @pl.when(c < cols - 1)
        def _(copy=copy, u=u):
            psend[u] = (fades[rows, u, 0:1, :] * pin[u].astype(F32) + before[rows, u]).astype(BF16)
            copy.start()

        for d in range(1, rows):
            q = lax.rem(r + d, rows)
            esend[d, u] = (fades[q, u, 0:1, :] * pin[u].astype(F32) + before[q, u]).astype(BF16)
            copy = pltpu.make_async_remote_copy(
                src_ref=esend.at[d, u],
                dst_ref=enter_ref.at[r, u],
                send_sem=s3.at[d, u],
                recv_sem=r3.at[d, u],
                device_id={"row": q},
                device_id_type=MESH,
            )
            copy.start()
            third.append(copy)
        enter_ref[r, u] = (fades[r, u, 0:1, :] * pin[u].astype(F32) + before[r, u]).astype(BF16)
    for copy in third:
        copy.wait()

    @pl.when(c < cols - 1)
    def _():
        for copy in second:
            copy.wait_send()


def finish_kernel(
    head_count, y_ref, gate_ref, outward_ref, ef_ref, enter_ref, gain_ref, wout_ref, result_ref, mix
):
    pieces, _, _, width = enter_ref.shape
    inner = pieces * width
    head_size = inner // head_count
    squares = None
    for q in range(pieces):
        far = jnp.dot(outward_ref[...], enter_ref[q, 0], preferred_element_type=F32)
        for j in range(width // head_size):
            h = q * (width // head_size) + j
            span = slice(h * head_size, (h + 1) * head_size)
            both = y_ref[:, span] + far[:, j * head_size : (j + 1) * head_size] * ef_ref[:, h : h + 1]
            value = both * silu(gate_ref[:, span].astype(F32))
            mix[:, span] = value
            squares = value * value if squares is None else squares + value * value
    mean = jnp.sum(squares, axis=1, keepdims=True) * (1.0 / inner)
    normed = (mix[...] * lax.rsqrt(mean + 1.0) * gain_ref[...]).astype(BF16)
    result = jnp.dot(normed, wout_ref[...], preferred_element_type=F32)
    result_ref[...] = (result * ef_ref[:, LANES - 1 : LANES]).astype(BF16)


def per_device(
    item_ids,
    pad_masks,
    lengths,
    item_table,
    w_gate,
    w_in,
    w_dt,
    conv_taps,
    dt_bias,
    decay_rates,
    norm_gain,
    w_out,
):
    users = item_ids.shape[0]
    events = item_ids.shape[2]
    items, model = item_table.shape
    full_width = w_in.shape[1]
    inner = w_gate.shape[1]
    head_count = decay_rates.shape[0]
    head_size = inner // head_count
    state_width = (full_width - inner) // 2
    rows, cols = lax.axis_size("row"), lax.axis_size("col")
    row_place, col_place = lax.axis_index("row"), lax.axis_index("col")
    stretch_count = events // STRETCH
    steps = users * stretch_count
    width = inner // rows

    item_rows = item_ids[:, 0, :]
    order = [r * cols + c for c in range(cols) for r in range(rows)]
    route = list(zip(order[:-1], order[1:]))
    halo = lax.ppermute(item_rows[:, events - HALO :] + 1, ("row", "col"), route) - 1
    first_event = (col_place * rows + row_place) * events
    position = first_event + lax.broadcasted_iota(jnp.int32, (users, events), 1)
    usable = jnp.logical_and(position < lengths[:, None], pad_masks[:, 0, :] > 0)
    joined = jnp.concatenate([halo, item_rows], axis=1).astype(F32)
    padded = 2 * STRETCH
    windows = jnp.stack(
        [joined[:, c * STRETCH : c * STRETCH + HALO + STRETCH] for c in range(stretch_count)], axis=1
    )
    windows = jnp.pad(windows, ((0, 0), (0, 0), (0, padded - HALO - STRETCH)))
    flags = jnp.pad(
        usable.astype(F32).reshape(users, stretch_count, STRETCH),
        ((0, 0), (0, 0), (0, padded - STRETCH)),
    )
    meta = jnp.pad(jnp.stack([windows, flags], axis=2), ((0, 0), (0, 0), (0, 6), (0, 0)))
    meta = meta.reshape(steps, 8, padded)

    table_in = jnp.dot(item_table, w_in, preferred_element_type=F32).astype(BF16)
    table_gate = jnp.dot(item_table, w_gate, preferred_element_type=F32).astype(BF16)
    raw = jnp.dot(item_table, w_dt, preferred_element_type=F32)
    high = lax.reduce_precision(raw, 8, 7)
    middle = lax.reduce_precision(raw - high, 8, 7)
    low = raw - high - middle
    table_dt = jnp.concatenate([high, middle, low], axis=1).astype(BF16)
    table_dt = jnp.pad(table_dt, ((0, 0), (0, LANES - 3 * head_count)))
    bias = jnp.pad(dt_bias[None], ((0, 0), (0, LANES - head_count)))
    rates = jnp.pad(decay_rates[None], ((0, 0), (0, LANES - head_count)))

    def whole(shape):
        return pl.BlockSpec(shape, lambda s: (0,) * len(shape))

    def by_rows(columns):
        return pl.BlockSpec((STRETCH, columns), lambda s: (s, 0))

    total_rows = users * events
    y, gate, outward, ef, state, logs = pl.pallas_call(
        functools.partial(
            local_kernel, (stretch_count, head_count, head_size, state_width, rows)
        ),
        grid=(steps,),
        in_specs=[
            pl.BlockSpec((1, 8, padded), lambda s: (s, 0, 0)),
            whole((items, full_width)),
            whole((items, inner)),
            whole((items, LANES)),
            whole(conv_taps.shape),
            whole((1, LANES)),
            whole((1, LANES)),
        ],
        out_specs=[
            by_rows(inner),
            by_rows(inner),
            by_rows(state_width),
            by_rows(LANES),
            pl.BlockSpec((rows, 1, state_width, width), lambda s: (0, s // stretch_count, 0, 0)),
            pl.BlockSpec((rows, 1, 8, width), lambda s: (0, s // stretch_count, 0, 0)),
        ],
        out_shape=[
            jax.ShapeDtypeStruct((total_rows, inner), F32),
            jax.ShapeDtypeStruct((total_rows, inner), BF16),
            jax.ShapeDtypeStruct((total_rows, state_width), BF16),
            jax.ShapeDtypeStruct((total_rows, LANES), F32),
            jax.ShapeDtypeStruct((rows, users, state_width, width), BF16),
            jax.ShapeDtypeStruct((rows, users, 8, width), F32),
        ],
        scratch_shapes=[
            pltpu.VMEM((HALO + STRETCH, full_width), F32),
            pltpu.VMEM((STRETCH, inner), BF16),
            pltpu.VMEM((state_width, inner), F32),
            pltpu.VMEM((8, LANES), F32),
        ],
        compiler_params=pltpu.CompilerParams(dimension_semantics=("arbitrary",)),
        name="local_part",
    )(meta, table_in, table_gate, table_dt, conv_taps, bias, rates)

    vmem = pl.BlockSpec(memory_space=pltpu.VMEM)
    dma = pltpu.SemaphoreType.DMA
    entering = pl.pallas_call(
        functools.partial(chain_kernel, rows, cols),
        in_specs=[vmem, vmem],
        out_specs=vmem,
        out_shape=jax.ShapeDtypeStruct(state.shape, BF16),
        scratch_shapes=[
            pltpu.VMEM(state.shape, BF16),
            pltpu.VMEM(logs.shape, F32),
            pltpu.VMEM((rows + 1,) + state.shape[1:], F32),
            pltpu.VMEM((rows + 1,) + logs.shape[1:], F32),
            pltpu.VMEM(state.shape[1:], BF16),
            pltpu.VMEM(state.shape[1:], BF16),
            pltpu.VMEM(state.shape, BF16),
            dma((rows,)),
            dma((rows,)),
            dma((rows,)),
            dma((rows,)),
            dma((users,)),
            dma((users,)),
            dma((rows, users)),
            dma((rows, users)),
        ],
        compiler_params=pltpu.CompilerParams(collective_id=0, has_side_effects=True),
        name="state_chain",
    )(state, logs)

    result = pl.pallas_call(
        functools.partial(finish_kernel, head_count),
        grid=(steps,),
        in_specs=[
            by_rows(inner),
            by_rows(inner),
            by_rows(state_width),
            by_rows(LANES),
            pl.BlockSpec((rows, 1, state_width, width), lambda s: (0, s // stretch_count, 0, 0)),
            whole((1, inner)),
            whole(w_out.shape),
        ],
        out_specs=by_rows(w_out.shape[1]),
        out_shape=jax.ShapeDtypeStruct((total_rows, w_out.shape[1]), BF16),
        scratch_shapes=[pltpu.VMEM((STRETCH, inner), F32)],
        compiler_params=pltpu.CompilerParams(dimension_semantics=("arbitrary",)),
        name="finish_part",
    )(y, gate, outward, ef, entering, norm_gain[None], w_out)
    return result.reshape(users, 1, events, -1)


def solution(mesh):
    in_specs = (
        P("batch", "col", "row"),
        P("batch", "col", "row"),
        P("batch"),
        P(),
        P(),
        P(),
        P(),
        P(),
        P(),
        P(),
        P(),
        P(),
    )
    out_specs = P("batch", "col", "row", None)
    return jax.shard_map(
        per_device, mesh=mesh, in_specs=in_specs, out_specs=out_specs, check_vma=False
    )
```

```python
import functools

import jax
import jax.numpy as jnp
from jax import lax
from jax.experimental import pallas as pl
from jax.experimental.pallas import tpu as pltpu
from jax.sharding import PartitionSpec as P

STRETCH = 128
LANES = 128
HALO = 16
MESH = pl.DeviceIdType.MESH
F32 = jnp.float32
BF16 = jnp.bfloat16


def silu(v):
    return 0.5 * v * (1.0 + jnp.tanh(0.5 * v))


def project_kernel(
    counts, table_ref, win_ref, wgate_ref, wdt_ref, tin_ref, tgate_ref, tdt_ref, wide
):
    in_blocks, gate_blocks, head_count = counts
    step = pl.program_id(0)

    @pl.when(step < in_blocks)
    def _():
        tin_ref[...] = jnp.dot(
            table_ref[...], win_ref[...], preferred_element_type=F32
        ).astype(BF16)

    @pl.when(step < gate_blocks)
    def _():
        tgate_ref[...] = jnp.dot(
            table_ref[...], wgate_ref[...], preferred_element_type=F32
        ).astype(BF16)

    @pl.when(step == pl.num_programs(0) - 1)
    def _():
        wide[...] = jnp.zeros_like(wide)
        wide[:, 0:head_count] = wdt_ref[...]
        raw = jnp.dot(table_ref[...], wide[...], preferred_element_type=F32)
        high = raw.astype(BF16).astype(F32)
        middle = (raw - high).astype(BF16).astype(F32)
        low = raw - high - middle
        tdt_ref[...] = (
            high + pltpu.roll(middle, head_count, 1) + pltpu.roll(low, 2 * head_count, 1)
        ).astype(BF16)


def local_kernel(
    counts,
    lengths_ref,
    ids_ref,
    halo_ref,
    masks_ref,
    tin_ref,
    tgate_ref,
    tdt_ref,
    taps_ref,
    bias_ref,
    rates_ref,
    y_ref,
    gate_ref,
    out_ref,
    ef_ref,
    state_ref,
    log_ref,
    rowbuf,
    pbuf,
    partbuf,
    usebuf,
    wide,
    scaled,
    run,
    cum,
):
    stretch_count, head_count, head_size, state_width, pieces = counts
    inner = head_count * head_size
    place = lax.rem(pl.program_id(0), stretch_count)
    user = pl.program_id(0) // stretch_count
    events = stretch_count * STRETCH

    @pl.when(place == 0)
    def _():
        run[...] = jnp.zeros_like(run)
        cum[...] = jnp.zeros_like(cum)
        wide[...] = jnp.zeros_like(wide)
        wide[0:1, 0:head_count] = bias_ref[...]
        wide[1:2, 0:head_count] = rates_ref[...]
        first = (lax.axis_index("col") * pieces + lax.axis_index("row")) * events
        halo = jnp.where(first == 0, -1, halo_ref[0])
        names = jnp.concatenate([halo, ids_ref[0]], axis=1).astype(F32)
        position = first + lax.broadcasted_iota(jnp.int32, (1, events), 1)
        kept = jnp.where(position < lengths_ref[user], masks_ref[0], 0)
        kept = jnp.where(kept > 0, 1.0, 0.0).astype(F32)
        flags = jnp.concatenate([jnp.zeros((1, STRETCH), F32), kept], axis=1)
        line = lax.broadcasted_iota(jnp.int32, (8, STRETCH + events), 0)
        meta = jnp.transpose(jnp.where(line == 0, names, jnp.where(line == 1, flags, 0.0)))
        usebuf[...] = meta[STRETCH:, :]
        ids = meta[STRETCH - HALO :, 0:1].astype(jnp.int32)
        items = tin_ref.shape[0]
        lane = lax.broadcasted_iota(jnp.int32, (HALO + events, items), 1)
        hot = (ids == lane).astype(F32).astype(BF16)
        rowbuf[...] = jnp.dot(hot, tin_ref[...], preferred_element_type=F32)
        now = hot[HALO:]
        gate_ref[...] = jnp.dot(now, tgate_ref[...], preferred_element_type=F32).astype(BF16)
        partbuf[...] = jnp.dot(now, tdt_ref[...], preferred_element_type=F32)

    base = pl.multiple_of(place * STRETCH, STRETCH)
    pbuf[...] = rowbuf[pl.ds(base, HALO + STRETCH), :]
    usable = usebuf[pl.ds(base, STRETCH), :][:, 1:2]
    parts = partbuf[pl.ds(base, STRETCH), :]
    raw = (
        parts
        + pltpu.roll(parts, LANES - head_count, 1)
        + pltpu.roll(parts, LANES - 2 * head_count, 1)
    )
    raw = raw + wide[0:1, :]
    step = usable * (jnp.maximum(raw, 0.0) + jnp.log1p(jnp.exp(-jnp.abs(raw))))
    rows = lax.broadcasted_iota(jnp.int32, (STRETCH, STRETCH), 0)
    cols = lax.broadcasted_iota(jnp.int32, (STRETCH, STRETCH), 1)
    causal = rows >= cols
    logs = jnp.dot(
        jnp.where(causal, 1.0, 0.0).astype(F32),
        step * wide[1:2, :],
        precision=lax.Precision.HIGHEST,
        preferred_element_type=F32,
    )
    total = logs[STRETCH - 1 :, :]
    logs_t = jnp.transpose(logs)
    step_t = jnp.transpose(step)
    kernel = taps_ref.shape[0]
    conv = None
    for k in range(kernel):
        start = HALO - (kernel - 1) + k
        term = pbuf[start : start + STRETCH, :] * taps_ref[k : k + 1, :]
        conv = term if conv is None else conv + term
    signal = silu(conv[:, :inner]).astype(BF16)
    inward = conv[:, inner : inner + state_width].astype(BF16)
    outward = conv[:, inner + state_width :].astype(BF16)
    out_ref[...] = outward
    scores = lax.dot_general(
        outward, inward, (((1,), (1,)), ((), ())), preferred_element_type=F32
    )
    scores = jnp.where(causal, scores, 0.0)
    tail = jnp.exp(logs - total) * step
    fade = jnp.exp(-logs)
    held = jnp.dot(outward, run[...].astype(BF16), preferred_element_type=F32)
    for h in range(head_count):
        span = slice(h * head_size, (h + 1) * head_size)
        gap = jnp.minimum(logs_t[h : h + 1, :] - logs[:, h : h + 1], 0.0)
        weights = (jnp.exp(gap) * (scores * step_t[h : h + 1, :])).astype(BF16)
        near = jnp.dot(weights, signal[:, span], preferred_element_type=F32)
        y_ref[:, span] = near + held[:, span] * fade[:, h : h + 1]
        scaled[:, span] = (signal[:, span].astype(F32) * tail[:, h : h + 1]).astype(BF16)
    added = lax.dot_general(
        inward, scaled[...], (((0,), (0,)), ((), ())), preferred_element_type=F32
    )
    shrink = jnp.exp(-total)
    for h in range(head_count):
        span = slice(h * head_size, (h + 1) * head_size)
        run[:, span] = run[:, span] * shrink[:, h : h + 1] + added[:, span]
    before = cum[0:1, :]
    lane = lax.broadcasted_iota(jnp.int32, (STRETCH, LANES), 1)
    ef_ref[...] = jnp.where(lane == LANES - 1, usable, jnp.exp(-(logs + before)))
    after = before + total
    cum[...] = jnp.broadcast_to(after, cum.shape)

    @pl.when(place == stretch_count - 1)
    def _():
        width = inner // pieces
        for q in range(pieces):
            state_ref[q, 0] = run[:, q * width : (q + 1) * width].astype(BF16)
            for j in range(width // head_size):
                h = q * (width // head_size) + j
                log_ref[q, 0, :, j * head_size : (j + 1) * head_size] = jnp.broadcast_to(
                    after[:, h : h + 1], (8, head_size)
                )


def chain_kernel(
    rows,
    cols,
    state_ref,
    log_ref,
    enter_ref,
    rin,
    lin,
    before,
    fades,
    pin,
    psend,
    esend,
    s1,
    r1,
    sl,
    rl,
    s2,
    r2,
    s3,
    r3,
):
    users = state_ref.shape[1]
    r, c = lax.axis_index("row"), lax.axis_index("col")
    barrier = pltpu.get_barrier_semaphore()
    for d in range(1, rows):
        pl.semaphore_signal(
            barrier, inc=1, device_id={"row": lax.rem(r + d, rows)}, device_id_type=MESH
        )

    @pl.when(c > 0)
    def _():
        pl.semaphore_signal(barrier, inc=1, device_id={"col": c - 1}, device_id_type=MESH)

    @pl.when(c < cols - 1)
    def _():
        pl.semaphore_signal(barrier, inc=1, device_id={"col": c + 1}, device_id_type=MESH)

    peers = rows - 1 + jnp.where(c > 0, 1, 0) + jnp.where(c < cols - 1, 1, 0)
    pl.semaphore_wait(barrier, peers)

    first = []
    for d in range(1, rows):
        q = lax.rem(r + d, rows)
        for source, target, send, recv in (
            (log_ref, lin, sl, rl),
            (state_ref, rin, s1, r1),
        ):
            copy = pltpu.make_async_remote_copy(
                src_ref=source.at[q],
                dst_ref=target.at[r],
                send_sem=send.at[d],
                recv_sem=recv.at[d],
                device_id={"row": q},
                device_id_type=MESH,
            )
            copy.start()
            first.append(copy)
    rin[r] = state_ref[r]
    lin[r] = log_ref[r]
    for copy in first:
        copy.wait()

    for u in range(users):
        carried = jnp.zeros(pin.shape[1:], F32)
        fade = jnp.ones((1, pin.shape[2]), F32)
        for m in range(rows):
            before[m, u] = carried
            fades[m, u] = jnp.broadcast_to(fade, fades.shape[2:])
            here = jnp.exp(-lin[m, u, 0:1, :])
            carried = here * carried + rin[m, u].astype(F32)
            fade = fade * here
        before[rows, u] = carried
        fades[rows, u] = jnp.broadcast_to(fade, fades.shape[2:])

    @pl.when(c == 0)
    def _():
        pin[...] = jnp.zeros_like(pin)

    second = []
    third = []
    for u in range(users):
        copy = pltpu.make_async_remote_copy(
            src_ref=psend.at[u],
            dst_ref=pin.at[u],
            send_sem=s2.at[u],
            recv_sem=r2.at[u],
            device_id={"col": lax.rem(c + 1, cols)},
            device_id_type=MESH,
        )
        second.append(copy)

        @pl.when(c > 0)
        def _(copy=copy):
            copy.wait_recv()

        @pl.when(c < cols - 1)
        def _(copy=copy, u=u):
            psend[u] = (fades[rows, u, 0:1, :] * pin[u].astype(F32) + before[rows, u]).astype(BF16)
            copy.start()

        for d in range(1, rows):
            q = lax.rem(r + d, rows)
            esend[d, u] = (fades[q, u, 0:1, :] * pin[u].astype(F32) + before[q, u]).astype(BF16)
            copy = pltpu.make_async_remote_copy(
                src_ref=esend.at[d, u],
                dst_ref=enter_ref.at[r, u],
                send_sem=s3.at[d, u],
                recv_sem=r3.at[d, u],
                device_id={"row": q},
                device_id_type=MESH,
            )
            copy.start()
            third.append(copy)
        enter_ref[r, u] = (fades[r, u, 0:1, :] * pin[u].astype(F32) + before[r, u]).astype(BF16)
    for copy in third:
        copy.wait()

    @pl.when(c < cols - 1)
    def _():
        for copy in second:
            copy.wait_send()


def finish_kernel(
    head_count, y_ref, gate_ref, outward_ref, ef_ref, enter_ref, gain_ref, wout_ref, result_ref, mix
):
    pieces, _, _, width = enter_ref.shape
    inner = pieces * width
    head_size = inner // head_count
    squares = None
    for q in range(pieces):
        far = jnp.dot(outward_ref[...], enter_ref[q, 0], preferred_element_type=F32)
        for j in range(width // head_size):
            h = q * (width // head_size) + j
            span = slice(h * head_size, (h + 1) * head_size)
            both = y_ref[:, span] + far[:, j * head_size : (j + 1) * head_size] * ef_ref[:, h : h + 1]
            value = both * silu(gate_ref[:, span].astype(F32))
            mix[:, span] = value
            squares = value * value if squares is None else squares + value * value
    mean = jnp.sum(squares, axis=1, keepdims=True) * (1.0 / inner)
    normed = (mix[...] * lax.rsqrt(mean + 1.0) * gain_ref[...]).astype(BF16)
    result = jnp.dot(normed, wout_ref[...], preferred_element_type=F32)
    result_ref[...] = (result * ef_ref[:, LANES - 1 : LANES]).astype(BF16)


def per_device(
    item_ids,
    pad_masks,
    lengths,
    item_table,
    w_gate,
    w_in,
    w_dt,
    conv_taps,
    dt_bias,
    decay_rates,
    norm_gain,
    w_out,
):
    users = item_ids.shape[0]
    events = item_ids.shape[2]
    items, model = item_table.shape
    full_width = w_in.shape[1]
    inner = w_gate.shape[1]
    head_count = decay_rates.shape[0]
    head_size = inner // head_count
    state_width = (full_width - inner) // 2
    rows, cols = lax.axis_size("row"), lax.axis_size("col")
    stretch_count = events // STRETCH
    steps = users * stretch_count
    width = inner // rows

    order = [r * cols + c for c in range(cols) for r in range(rows)]
    route = list(zip(order[:-1], order[1:]))
    halo = lax.ppermute(item_ids[:, :, events - STRETCH :], ("row", "col"), route)

    def whole(shape):
        return pl.BlockSpec(shape, lambda s: (0,) * len(shape))

    def by_rows(columns):
        return pl.BlockSpec((STRETCH, columns), lambda s: (s, 0))

    total_rows = users * events
    block = 2 * LANES
    in_blocks, gate_blocks = full_width // block, inner // block
    table_in, table_gate, table_dt = pl.pallas_call(
        functools.partial(project_kernel, (in_blocks, gate_blocks, head_count)),
        grid=(max(in_blocks, gate_blocks),),
        in_specs=[
            whole((items, model)),
            pl.BlockSpec((model, block), lambda s: (0, jnp.minimum(s, in_blocks - 1))),
            pl.BlockSpec((model, block), lambda s: (0, jnp.minimum(s, gate_blocks - 1))),
            whole(w_dt.shape),
        ],
        out_specs=[
            pl.BlockSpec((items, block), lambda s: (0, jnp.minimum(s, in_blocks - 1))),
            pl.BlockSpec((items, block), lambda s: (0, jnp.minimum(s, gate_blocks - 1))),
            whole((items, LANES)),
        ],
        out_shape=[
            jax.ShapeDtypeStruct((items, full_width), BF16),
            jax.ShapeDtypeStruct((items, inner), BF16),
            jax.ShapeDtypeStruct((items, LANES), BF16),
        ],
        scratch_shapes=[pltpu.VMEM((model, LANES), BF16)],
        compiler_params=pltpu.CompilerParams(dimension_semantics=("arbitrary",)),
        cost_estimate=pl.CostEstimate(
            flops=2 * items * model * (full_width + inner),
            bytes_accessed=4 * model * (full_width + inner),
            transcendentals=0,
        ),
        name="table_part",
    )(item_table, w_in, w_gate, w_dt)

    def by_user(columns):
        return pl.BlockSpec((1, 1, columns), lambda s: (s // stretch_count, 0, 0))

    y, gate, outward, ef, state, logs = pl.pallas_call(
        functools.partial(
            local_kernel, (stretch_count, head_count, head_size, state_width, rows)
        ),
        grid=(steps,),
        in_specs=[
            pl.BlockSpec(memory_space=pltpu.SMEM),
            by_user(events),
            by_user(STRETCH),
            by_user(events),
            whole((items, full_width)),
            whole((items, inner)),
            whole((items, LANES)),
            whole(conv_taps.shape),
            whole((1, head_count)),
            whole((1, head_count)),
        ],
        out_specs=[
            by_rows(inner),
            pl.BlockSpec((events, inner), lambda s: (s // stretch_count, 0)),
            by_rows(state_width),
            by_rows(LANES),
            pl.BlockSpec((rows, 1, state_width, width), lambda s: (0, s // stretch_count, 0, 0)),
            pl.BlockSpec((rows, 1, 8, width), lambda s: (0, s // stretch_count, 0, 0)),
        ],
        out_shape=[
            jax.ShapeDtypeStruct((total_rows, inner), F32),
            jax.ShapeDtypeStruct((total_rows, inner), BF16),
            jax.ShapeDtypeStruct((total_rows, state_width), BF16),
            jax.ShapeDtypeStruct((total_rows, LANES), F32),
            jax.ShapeDtypeStruct((rows, users, state_width, width), BF16),
            jax.ShapeDtypeStruct((rows, users, 8, width), F32),
        ],
        scratch_shapes=[
            pltpu.VMEM((HALO + events, full_width), F32),
            pltpu.VMEM((HALO + STRETCH, full_width), F32),
            pltpu.VMEM((events, LANES), F32),
            pltpu.VMEM((events, 8), F32),
            pltpu.VMEM((8, LANES), F32),
            pltpu.VMEM((STRETCH, inner), BF16),
            pltpu.VMEM((state_width, inner), F32),
            pltpu.VMEM((8, LANES), F32),
        ],
        compiler_params=pltpu.CompilerParams(dimension_semantics=("arbitrary",)),
        name="local_part",
    )(
        lengths,
        item_ids,
        halo,
        pad_masks,
        table_in,
        table_gate,
        table_dt,
        conv_taps,
        dt_bias[None],
        decay_rates[None],
    )

    vmem = pl.BlockSpec(memory_space=pltpu.VMEM)
    dma = pltpu.SemaphoreType.DMA
    entering = pl.pallas_call(
        functools.partial(chain_kernel, rows, cols),
        in_specs=[vmem, vmem],
        out_specs=vmem,
        out_shape=jax.ShapeDtypeStruct(state.shape, BF16),
        scratch_shapes=[
            pltpu.VMEM(state.shape, BF16),
            pltpu.VMEM(logs.shape, F32),
            pltpu.VMEM((rows + 1,) + state.shape[1:], F32),
            pltpu.VMEM((rows + 1,) + logs.shape[1:], F32),
            pltpu.VMEM(state.shape[1:], BF16),
            pltpu.VMEM(state.shape[1:], BF16),
            pltpu.VMEM(state.shape, BF16),
            dma((rows,)),
            dma((rows,)),
            dma((rows,)),
            dma((rows,)),
            dma((users,)),
            dma((users,)),
            dma((rows, users)),
            dma((rows, users)),
        ],
        compiler_params=pltpu.CompilerParams(collective_id=0, has_side_effects=True),
        name="state_chain",
    )(state, logs)

    tall = 2 * STRETCH if events % (2 * STRETCH) == 0 else STRETCH

    def tall_rows(columns):
        return pl.BlockSpec((tall, columns), lambda s: (s, 0))

    result = pl.pallas_call(
        functools.partial(finish_kernel, head_count),
        grid=(total_rows // tall,),
        in_specs=[
            tall_rows(inner),
            tall_rows(inner),
            tall_rows(state_width),
            tall_rows(LANES),
            pl.BlockSpec((rows, 1, state_width, width), lambda s: (0, s // (events // tall), 0, 0)),
            whole((1, inner)),
            whole(w_out.shape),
        ],
        out_specs=tall_rows(w_out.shape[1]),
        out_shape=jax.ShapeDtypeStruct((total_rows, w_out.shape[1]), BF16),
        scratch_shapes=[pltpu.VMEM((tall, inner), F32)],
        compiler_params=pltpu.CompilerParams(dimension_semantics=("arbitrary",)),
        name="finish_part",
    )(y, gate, outward, ef, entering, norm_gain[None], w_out)
    return result.reshape(users, 1, events, -1)


def solution(mesh):
    in_specs = (
        P("batch", "col", "row"),
        P("batch", "col", "row"),
        P("batch"),
        P(),
        P(),
        P(),
        P(),
        P(),
        P(),
        P(),
        P(),
        P(),
    )
    out_specs = P("batch", "col", "row", None)
    return jax.shard_map(
        per_device, mesh=mesh, in_specs=in_specs, out_specs=out_specs, check_vma=False
    )
```

```python
import functools

import jax
import jax.numpy as jnp
from jax import lax
from jax.experimental import pallas as pl
from jax.experimental.pallas import tpu as pltpu
from jax.sharding import PartitionSpec as P

STRETCH = 128
LANES = 128
HALO = 16
MESH = pl.DeviceIdType.MESH
F32 = jnp.float32
BF16 = jnp.bfloat16


def silu(v):
    return 0.5 * v * (1.0 + jnp.tanh(0.5 * v))


def project_kernel(
    counts,
    mesh_sizes,
    ids_ref,
    table_ref,
    win_ref,
    wgate_ref,
    wdt_ref,
    tin_ref,
    tgate_ref,
    tdt_ref,
    halo_ref,
    wide,
    landed,
    send_sem,
    recv_sem,
):
    rows, cols = mesh_sizes
    r, c = lax.axis_index("row"), lax.axis_index("col")
    place = c * rows + r
    later = lax.rem(place + 1, rows * cols)
    earlier = lax.rem(place + rows * cols - 1, rows * cols)
    after = {"row": lax.rem(later, rows), "col": later // rows}
    ahead = {"row": lax.rem(earlier, rows), "col": earlier // rows}
    has_after, has_before = place < rows * cols - 1, place > 0
    barrier = pltpu.get_barrier_semaphore()
    events = ids_ref.shape[2]
    copy = pltpu.make_async_remote_copy(
        src_ref=ids_ref.at[:, :, pl.ds(events - STRETCH, STRETCH)],
        dst_ref=landed,
        send_sem=send_sem,
        recv_sem=recv_sem,
        device_id=after,
        device_id_type=MESH,
    )
    begin = pl.program_id(0) == 0

    @pl.when(jnp.logical_and(begin, has_before))
    def _():
        pl.semaphore_signal(barrier, inc=1, device_id=ahead, device_id_type=MESH)

    @pl.when(jnp.logical_and(begin, has_after))
    def _():
        pl.semaphore_signal(barrier, inc=1, device_id=after, device_id_type=MESH)

    @pl.when(pl.program_id(0) == 1)
    def _():
        peers = jnp.where(has_before, 1, 0) + jnp.where(has_after, 1, 0)
        pl.semaphore_wait(barrier, peers)

        @pl.when(has_after)
        def _():
            copy.start()

    in_blocks, gate_blocks, head_count = counts
    step = pl.program_id(0)

    @pl.when(step < in_blocks)
    def _():
        tin_ref[...] = jnp.dot(
            table_ref[...], win_ref[...], preferred_element_type=F32
        ).astype(BF16)

    @pl.when(step < gate_blocks)
    def _():
        tgate_ref[...] = jnp.dot(
            table_ref[...], wgate_ref[...], preferred_element_type=F32
        ).astype(BF16)

    @pl.when(step == pl.num_programs(0) - 1)
    def _():
        wide[...] = jnp.zeros_like(wide)
        wide[0:head_count, :] = wdt_ref[...]
        raw = lax.dot_general(
            table_ref[...], wide[...], (((1,), (1,)), ((), ())), preferred_element_type=F32
        )
        high = raw.astype(BF16).astype(F32)
        middle = (raw - high).astype(BF16).astype(F32)
        low = raw - high - middle
        tdt_ref[...] = (
            high + pltpu.roll(middle, head_count, 1) + pltpu.roll(low, 2 * head_count, 1)
        ).astype(BF16)

        @pl.when(has_after)
        def _():
            copy.wait_send()

        @pl.when(has_before)
        def _():
            copy.wait_recv()
            halo_ref[...] = landed[...]

        @pl.when(place == 0)
        def _():
            halo_ref[...] = jnp.full(halo_ref.shape, -1, jnp.int32)


def local_kernel(
    counts,
    lengths_ref,
    ids_ref,
    halo_ref,
    masks_ref,
    tin_ref,
    tgate_ref,
    tdt_ref,
    taps_ref,
    bias_ref,
    rates_ref,
    y_ref,
    gate_ref,
    out_ref,
    ef_ref,
    state_ref,
    log_ref,
    rowbuf,
    pbuf,
    partbuf,
    usebuf,
    wide,
    scaled,
    run,
    cum,
):
    stretch_count, head_count, head_size, state_width, pieces = counts
    inner = head_count * head_size
    place = lax.rem(pl.program_id(0), stretch_count)
    user = pl.program_id(0) // stretch_count
    events = stretch_count * STRETCH

    @pl.when(place == 0)
    def _():
        run[...] = jnp.zeros_like(run)
        cum[...] = jnp.zeros_like(cum)
        wide[...] = jnp.zeros_like(wide)
        wide[0:1, 0:head_count] = bias_ref[...]
        wide[1:2, 0:head_count] = rates_ref[...]
        first = (lax.axis_index("col") * pieces + lax.axis_index("row")) * events
        halo = jnp.where(first == 0, -1, halo_ref[0])
        names = jnp.concatenate([halo, ids_ref[0]], axis=1).astype(F32)
        position = first + lax.broadcasted_iota(jnp.int32, (1, events), 1)
        kept = jnp.where(position < lengths_ref[user], masks_ref[0], 0)
        kept = jnp.where(kept > 0, 1.0, 0.0).astype(F32)
        flags = jnp.concatenate([jnp.zeros((1, STRETCH), F32), kept], axis=1)
        line = lax.broadcasted_iota(jnp.int32, (8, STRETCH + events), 0)
        meta = jnp.transpose(jnp.where(line == 0, names, jnp.where(line == 1, flags, 0.0)))
        usebuf[...] = meta[STRETCH:, :]
        ids = meta[STRETCH - HALO :, 0:1].astype(jnp.int32)
        items = tin_ref.shape[0]
        lane = lax.broadcasted_iota(jnp.int32, (HALO + events, items), 1)
        hot = (ids == lane).astype(F32).astype(BF16)
        rowbuf[...] = jnp.dot(hot, tin_ref[...], preferred_element_type=F32)
        now = hot[HALO:]
        gate_ref[...] = jnp.dot(now, tgate_ref[...], preferred_element_type=F32).astype(BF16)
        partbuf[...] = jnp.dot(now, tdt_ref[...], preferred_element_type=F32)

    base = pl.multiple_of(place * STRETCH, STRETCH)
    pbuf[...] = rowbuf[pl.ds(base, HALO + STRETCH), :]
    usable = usebuf[pl.ds(base, STRETCH), :][:, 1:2]
    parts = partbuf[pl.ds(base, STRETCH), :]
    raw = (
        parts
        + pltpu.roll(parts, LANES - head_count, 1)
        + pltpu.roll(parts, LANES - 2 * head_count, 1)
    )
    raw = raw + wide[0:1, :]
    step = usable * (jnp.maximum(raw, 0.0) + jnp.log1p(jnp.exp(-jnp.abs(raw))))
    rows = lax.broadcasted_iota(jnp.int32, (STRETCH, STRETCH), 0)
    cols = lax.broadcasted_iota(jnp.int32, (STRETCH, STRETCH), 1)
    causal = rows >= cols
    logs = jnp.dot(
        jnp.where(causal, 1.0, 0.0).astype(F32),
        step * wide[1:2, :],
        precision=lax.Precision.HIGHEST,
        preferred_element_type=F32,
    )
    total = logs[STRETCH - 1 :, :]
    logs_t = jnp.transpose(logs)
    step_t = jnp.transpose(step)
    kernel = taps_ref.shape[0]
    conv = None
    for k in range(kernel):
        start = HALO - (kernel - 1) + k
        term = pbuf[start : start + STRETCH, :] * taps_ref[k : k + 1, :]
        conv = term if conv is None else conv + term
    signal = silu(conv[:, :inner]).astype(BF16)
    inward = conv[:, inner : inner + state_width].astype(BF16)
    outward = conv[:, inner + state_width :].astype(BF16)
    out_ref[...] = outward
    scores = lax.dot_general(
        outward, inward, (((1,), (1,)), ((), ())), preferred_element_type=F32
    )
    scores = jnp.where(causal, scores, 0.0)
    tail = jnp.exp(logs - total) * step
    fade = jnp.exp(-logs)
    held = jnp.dot(outward, run[...].astype(BF16), preferred_element_type=F32)
    for h in range(head_count):
        span = slice(h * head_size, (h + 1) * head_size)
        gap = jnp.minimum(logs_t[h : h + 1, :] - logs[:, h : h + 1], 0.0)
        weights = (jnp.exp(gap) * (scores * step_t[h : h + 1, :])).astype(BF16)
        near = jnp.dot(weights, signal[:, span], preferred_element_type=F32)
        y_ref[:, span] = (near + held[:, span] * fade[:, h : h + 1]).astype(BF16)
        scaled[:, span] = (signal[:, span].astype(F32) * tail[:, h : h + 1]).astype(BF16)
    added = lax.dot_general(
        inward, scaled[...], (((0,), (0,)), ((), ())), preferred_element_type=F32
    )
    shrink = jnp.exp(-total)
    for h in range(head_count):
        span = slice(h * head_size, (h + 1) * head_size)
        run[:, span] = run[:, span] * shrink[:, h : h + 1] + added[:, span]
    before = cum[0:1, :]
    lane = lax.broadcasted_iota(jnp.int32, (STRETCH, LANES), 1)
    ef_ref[...] = jnp.where(lane == LANES - 1, usable, jnp.exp(-(logs + before)))
    after = before + total
    cum[...] = jnp.broadcast_to(after, cum.shape)

    @pl.when(place == stretch_count - 1)
    def _():
        width = inner // pieces
        for q in range(pieces):
            state_ref[q, 0] = run[:, q * width : (q + 1) * width].astype(BF16)
            for j in range(width // head_size):
                h = q * (width // head_size) + j
                log_ref[q, 0, :, j * head_size : (j + 1) * head_size] = jnp.broadcast_to(
                    after[:, h : h + 1], (8, head_size)
                )


def chain_kernel(
    rows,
    cols,
    state_ref,
    log_ref,
    enter_ref,
    rin,
    lin,
    before,
    fades,
    pin,
    psend,
    esend,
    s1,
    r1,
    sl,
    rl,
    s2,
    r2,
    s3,
    r3,
):
    users = state_ref.shape[1]
    r, c = lax.axis_index("row"), lax.axis_index("col")
    barrier = pltpu.get_barrier_semaphore()
    for d in range(1, rows):
        pl.semaphore_signal(
            barrier, inc=1, device_id={"row": lax.rem(r + d, rows)}, device_id_type=MESH
        )

    @pl.when(c > 0)
    def _():
        pl.semaphore_signal(barrier, inc=1, device_id={"col": c - 1}, device_id_type=MESH)

    @pl.when(c < cols - 1)
    def _():
        pl.semaphore_signal(barrier, inc=1, device_id={"col": c + 1}, device_id_type=MESH)

    peers = rows - 1 + jnp.where(c > 0, 1, 0) + jnp.where(c < cols - 1, 1, 0)
    pl.semaphore_wait(barrier, peers)

    first = [[] for _ in range(users)]
    for u in range(users):
        for d in range(1, rows):
            q = lax.rem(r + d, rows)
            for source, target, send, recv in (
                (log_ref, lin, sl, rl),
                (state_ref, rin, s1, r1),
            ):
                copy = pltpu.make_async_remote_copy(
                    src_ref=source.at[q, u],
                    dst_ref=target.at[r, u],
                    send_sem=send.at[d, u],
                    recv_sem=recv.at[d, u],
                    device_id={"row": q},
                    device_id_type=MESH,
                )
                copy.start()
                first[u].append(copy)
    rin[r] = state_ref[r]
    lin[r] = log_ref[r]
    onward = [
        pltpu.make_async_remote_copy(
            src_ref=psend.at[u],
            dst_ref=pin.at[u],
            send_sem=s2.at[u],
            recv_sem=r2.at[u],
            device_id={"col": lax.rem(c + 1, cols)},
            device_id_type=MESH,
        )
        for u in range(users)
    ]

    for u in range(users):
        for copy in first[u]:
            copy.wait_recv()
        carried = jnp.zeros(pin.shape[1:], F32)
        fade = jnp.ones((1, pin.shape[2]), F32)
        for m in range(rows):
            before[m, u] = carried
            fades[m, u] = jnp.broadcast_to(fade, fades.shape[2:])
            here = jnp.exp(-lin[m, u, 0:1, :])
            carried = here * carried + rin[m, u].astype(F32)
            fade = fade * here
        before[rows, u] = carried
        fades[rows, u] = jnp.broadcast_to(fade, fades.shape[2:])
        if cols > 1:

            @pl.when(c == 0)
            def _(u=u, carried=carried):
                psend[u] = carried.astype(BF16)
                onward[u].start()

    @pl.when(c == 0)
    def _():
        pin[...] = jnp.zeros_like(pin)

    third = []
    for u in range(users):

        @pl.when(c > 0)
        def _(u=u):
            onward[u].wait_recv()

        @pl.when(jnp.logical_and(c > 0, c < cols - 1))
        def _(u=u):
            psend[u] = (fades[rows, u, 0:1, :] * pin[u].astype(F32) + before[rows, u]).astype(BF16)
            onward[u].start()

        for d in range(1, rows):
            q = lax.rem(r + d, rows)
            esend[d, u] = (fades[q, u, 0:1, :] * pin[u].astype(F32) + before[q, u]).astype(BF16)
            copy = pltpu.make_async_remote_copy(
                src_ref=esend.at[d, u],
                dst_ref=enter_ref.at[r, u],
                send_sem=s3.at[d, u],
                recv_sem=r3.at[d, u],
                device_id={"row": q},
                device_id_type=MESH,
            )
            copy.start()
            third.append(copy)
        enter_ref[r, u] = (fades[r, u, 0:1, :] * pin[u].astype(F32) + before[r, u]).astype(BF16)
    for copy in third:
        copy.wait()
    for group in first:
        for copy in group:
            copy.wait_send()

    @pl.when(c < cols - 1)
    def _():
        for copy in onward:
            copy.wait_send()


def finish_kernel(
    head_count, y_ref, gate_ref, outward_ref, ef_ref, enter_ref, gain_ref, wout_ref, result_ref, mix
):
    pieces, _, _, width = enter_ref.shape
    inner = pieces * width
    head_size = inner // head_count
    squares = None
    for q in range(pieces):
        far = jnp.dot(outward_ref[...], enter_ref[q, 0], preferred_element_type=F32)
        for j in range(width // head_size):
            h = q * (width // head_size) + j
            span = slice(h * head_size, (h + 1) * head_size)
            both = y_ref[:, span].astype(F32) + far[:, j * head_size : (j + 1) * head_size] * ef_ref[:, h : h + 1]
            value = both * silu(gate_ref[:, span].astype(F32))
            mix[:, span] = value
            squares = value * value if squares is None else squares + value * value
    mean = jnp.sum(squares, axis=1, keepdims=True) * (1.0 / inner)
    normed = (mix[...] * lax.rsqrt(mean + 1.0) * gain_ref[...]).astype(BF16)
    result = jnp.dot(normed, wout_ref[...], preferred_element_type=F32)
    result_ref[...] = (result * ef_ref[:, LANES - 1 : LANES]).astype(BF16)


def per_device(
    item_ids,
    pad_masks,
    lengths,
    item_table,
    w_gate,
    w_in,
    w_dt,
    conv_taps,
    dt_bias,
    decay_rates,
    norm_gain,
    w_out,
):
    users = item_ids.shape[0]
    events = item_ids.shape[2]
    items, model = item_table.shape
    full_width = w_in.shape[1]
    inner = w_gate.shape[1]
    head_count = decay_rates.shape[0]
    head_size = inner // head_count
    state_width = (full_width - inner) // 2
    rows, cols = lax.axis_size("row"), lax.axis_size("col")
    stretch_count = events // STRETCH
    steps = users * stretch_count
    width = inner // rows

    def whole(shape):
        return pl.BlockSpec(shape, lambda s: (0,) * len(shape))

    def by_rows(columns):
        return pl.BlockSpec((STRETCH, columns), lambda s: (s, 0))

    total_rows = users * events
    block = 2 * LANES
    in_blocks, gate_blocks = full_width // block, inner // block
    table_in, table_gate, table_dt, halo = pl.pallas_call(
        functools.partial(project_kernel, (in_blocks, gate_blocks, head_count), (rows, cols)),
        grid=(max(in_blocks, gate_blocks),),
        in_specs=[
            whole(item_ids.shape),
            whole((items, model)),
            pl.BlockSpec((model, block), lambda s: (0, jnp.minimum(s, in_blocks - 1))),
            pl.BlockSpec((model, block), lambda s: (0, jnp.minimum(s, gate_blocks - 1))),
            whole(w_dt.shape[::-1]),
        ],
        out_specs=[
            pl.BlockSpec((items, block), lambda s: (0, jnp.minimum(s, in_blocks - 1))),
            pl.BlockSpec((items, block), lambda s: (0, jnp.minimum(s, gate_blocks - 1))),
            whole((items, LANES)),
            whole((users, 1, STRETCH)),
        ],
        out_shape=[
            jax.ShapeDtypeStruct((items, full_width), BF16),
            jax.ShapeDtypeStruct((items, inner), BF16),
            jax.ShapeDtypeStruct((items, LANES), BF16),
            jax.ShapeDtypeStruct((users, 1, STRETCH), jnp.int32),
        ],
        scratch_shapes=[
            pltpu.VMEM((LANES, model), BF16),
            pltpu.VMEM((users, 1, STRETCH), jnp.int32),
            pltpu.SemaphoreType.DMA,
            pltpu.SemaphoreType.DMA,
        ],
        compiler_params=pltpu.CompilerParams(
            dimension_semantics=("arbitrary",), collective_id=1, has_side_effects=True
        ),
        cost_estimate=pl.CostEstimate(
            flops=2 * items * model * (full_width + inner),
            bytes_accessed=4 * model * (full_width + inner),
            transcendentals=0,
        ),
        name="table_part",
    )(item_ids, item_table, w_in, w_gate, w_dt.T)

    def by_user(columns):
        return pl.BlockSpec((1, 1, columns), lambda s: (s // stretch_count, 0, 0))

    y, gate, outward, ef, state, logs = pl.pallas_call(
        functools.partial(
            local_kernel, (stretch_count, head_count, head_size, state_width, rows)
        ),
        grid=(steps,),
        in_specs=[
            pl.BlockSpec(memory_space=pltpu.SMEM),
            by_user(events),
            by_user(STRETCH),
            by_user(events),
            whole((items, full_width)),
            whole((items, inner)),
            whole((items, LANES)),
            whole(conv_taps.shape),
            whole((1, head_count)),
            whole((1, head_count)),
        ],
        out_specs=[
            by_rows(inner),
            pl.BlockSpec((events, inner), lambda s: (s // stretch_count, 0)),
            by_rows(state_width),
            by_rows(LANES),
            pl.BlockSpec((rows, 1, state_width, width), lambda s: (0, s // stretch_count, 0, 0)),
            pl.BlockSpec((rows, 1, 8, width), lambda s: (0, s // stretch_count, 0, 0)),
        ],
        out_shape=[
            jax.ShapeDtypeStruct((total_rows, inner), BF16),
            jax.ShapeDtypeStruct((total_rows, inner), BF16),
            jax.ShapeDtypeStruct((total_rows, state_width), BF16),
            jax.ShapeDtypeStruct((total_rows, LANES), F32),
            jax.ShapeDtypeStruct((rows, users, state_width, width), BF16),
            jax.ShapeDtypeStruct((rows, users, 8, width), F32),
        ],
        scratch_shapes=[
            pltpu.VMEM((HALO + events, full_width), F32),
            pltpu.VMEM((HALO + STRETCH, full_width), F32),
            pltpu.VMEM((events, LANES), F32),
            pltpu.VMEM((events, 8), F32),
            pltpu.VMEM((8, LANES), F32),
            pltpu.VMEM((STRETCH, inner), BF16),
            pltpu.VMEM((state_width, inner), F32),
            pltpu.VMEM((8, LANES), F32),
        ],
        compiler_params=pltpu.CompilerParams(dimension_semantics=("arbitrary",)),
        name="local_part",
    )(
        lengths,
        item_ids,
        halo,
        pad_masks,
        table_in,
        table_gate,
        table_dt,
        conv_taps,
        dt_bias[None],
        decay_rates[None],
    )

    vmem = pl.BlockSpec(memory_space=pltpu.VMEM)
    dma = pltpu.SemaphoreType.DMA
    entering = pl.pallas_call(
        functools.partial(chain_kernel, rows, cols),
        in_specs=[vmem, vmem],
        out_specs=vmem,
        out_shape=jax.ShapeDtypeStruct(state.shape, BF16),
        scratch_shapes=[
            pltpu.VMEM(state.shape, BF16),
            pltpu.VMEM(logs.shape, F32),
            pltpu.VMEM((rows + 1,) + state.shape[1:], F32),
            pltpu.VMEM((rows + 1,) + logs.shape[1:], F32),
            pltpu.VMEM(state.shape[1:], BF16),
            pltpu.VMEM(state.shape[1:], BF16),
            pltpu.VMEM(state.shape, BF16),
            dma((rows, users)),
            dma((rows, users)),
            dma((rows, users)),
            dma((rows, users)),
            dma((users,)),
            dma((users,)),
            dma((rows, users)),
            dma((rows, users)),
        ],
        compiler_params=pltpu.CompilerParams(collective_id=0, has_side_effects=True),
        name="state_chain",
    )(state, logs)

    tall = 2 * STRETCH if events % (2 * STRETCH) == 0 else STRETCH

    def tall_rows(columns):
        return pl.BlockSpec((tall, columns), lambda s: (s, 0))

    result = pl.pallas_call(
        functools.partial(finish_kernel, head_count),
        grid=(total_rows // tall,),
        in_specs=[
            tall_rows(inner),
            tall_rows(inner),
            tall_rows(state_width),
            tall_rows(LANES),
            pl.BlockSpec((rows, 1, state_width, width), lambda s: (0, s // (events // tall), 0, 0)),
            whole((1, inner)),
            whole(w_out.shape),
        ],
        out_specs=tall_rows(w_out.shape[1]),
        out_shape=jax.ShapeDtypeStruct((total_rows, w_out.shape[1]), BF16),
        scratch_shapes=[pltpu.VMEM((tall, inner), F32)],
        compiler_params=pltpu.CompilerParams(dimension_semantics=("arbitrary",)),
        name="finish_part",
    )(y, gate, outward, ef, entering, norm_gain[None], w_out)
    return result.reshape(users, 1, events, -1)


def solution(mesh):
    in_specs = (
        P("batch", "col", "row"),
        P("batch", "col", "row"),
        P("batch"),
        P(),
        P(),
        P(),
        P(),
        P(),
        P(),
        P(),
        P(),
        P(),
    )
    out_specs = P("batch", "col", "row", None)
    return jax.shard_map(
        per_device, mesh=mesh, in_specs=in_specs, out_specs=out_specs, check_vma=False
    )
```

```python
import functools

import jax
import jax.numpy as jnp
from jax import lax
from jax.experimental import pallas as pl
from jax.experimental.pallas import tpu as pltpu
from jax.sharding import PartitionSpec as P

STRETCH = 128
LANES = 128
HALO = 16
MESH = pl.DeviceIdType.MESH
F32 = jnp.float32
BF16 = jnp.bfloat16


def silu(v):
    return 0.5 * v * (1.0 + jnp.tanh(0.5 * v))


def project_kernel(
    counts,
    mesh_sizes,
    ids_ref,
    table_ref,
    win_ref,
    wgate_ref,
    wdt_ref,
    tin_ref,
    tgate_ref,
    tdt_ref,
    halo_ref,
    wide,
    landed,
    send_sem,
    recv_sem,
):
    rows, cols = mesh_sizes
    r, c = lax.axis_index("row"), lax.axis_index("col")
    place = c * rows + r
    later = lax.rem(place + 1, rows * cols)
    earlier = lax.rem(place + rows * cols - 1, rows * cols)
    after = {"row": lax.rem(later, rows), "col": later // rows}
    ahead = {"row": lax.rem(earlier, rows), "col": earlier // rows}
    has_after, has_before = place < rows * cols - 1, place > 0
    barrier = pltpu.get_barrier_semaphore()
    events = ids_ref.shape[2]
    copy = pltpu.make_async_remote_copy(
        src_ref=ids_ref.at[:, :, pl.ds(events - STRETCH, STRETCH)],
        dst_ref=landed,
        send_sem=send_sem,
        recv_sem=recv_sem,
        device_id=after,
        device_id_type=MESH,
    )
    begin = pl.program_id(0) == 0

    @pl.when(jnp.logical_and(begin, has_before))
    def _():
        pl.semaphore_signal(barrier, inc=1, device_id=ahead, device_id_type=MESH)

    @pl.when(jnp.logical_and(begin, has_after))
    def _():
        pl.semaphore_signal(barrier, inc=1, device_id=after, device_id_type=MESH)

    @pl.when(pl.program_id(0) == 1)
    def _():
        peers = jnp.where(has_before, 1, 0) + jnp.where(has_after, 1, 0)
        pl.semaphore_wait(barrier, peers)

        @pl.when(has_after)
        def _():
            copy.start()

    in_blocks, gate_blocks, head_count = counts
    step = pl.program_id(0)

    @pl.when(step < in_blocks)
    def _():
        tin_ref[...] = jnp.dot(
            table_ref[...], win_ref[...], preferred_element_type=F32
        ).astype(BF16)

    @pl.when(step < gate_blocks)
    def _():
        tgate_ref[...] = jnp.dot(
            table_ref[...], wgate_ref[...], preferred_element_type=F32
        ).astype(BF16)

    @pl.when(step == pl.num_programs(0) - 1)
    def _():
        wide[...] = jnp.zeros_like(wide)
        wide[0:head_count, :] = wdt_ref[...]
        raw = lax.dot_general(
            table_ref[...], wide[...], (((1,), (1,)), ((), ())), preferred_element_type=F32
        )
        high = raw.astype(BF16).astype(F32)
        middle = (raw - high).astype(BF16).astype(F32)
        low = raw - high - middle
        tdt_ref[...] = (
            high + pltpu.roll(middle, head_count, 1) + pltpu.roll(low, 2 * head_count, 1)
        ).astype(BF16)

        @pl.when(has_after)
        def _():
            copy.wait_send()

        @pl.when(has_before)
        def _():
            copy.wait_recv()
            halo_ref[...] = landed[...]

        @pl.when(place == 0)
        def _():
            halo_ref[...] = jnp.full(halo_ref.shape, -1, jnp.int32)


def local_kernel(
    counts,
    lengths_ref,
    ids_ref,
    halo_ref,
    masks_ref,
    tin_ref,
    tgate_ref,
    tdt_ref,
    taps_ref,
    bias_ref,
    rates_ref,
    y_ref,
    gate_ref,
    out_ref,
    ef_ref,
    state_ref,
    log_ref,
    rowbuf,
    partbuf,
    usebuf,
    wide,
    scaled,
    run,
    cum,
):
    stretch_count, head_count, head_size, state_width, pieces = counts
    inner = head_count * head_size
    place = lax.rem(pl.program_id(0), stretch_count)
    user = pl.program_id(0) // stretch_count
    events = stretch_count * STRETCH

    @pl.when(place == 0)
    def _():
        run[...] = jnp.zeros_like(run)
        cum[...] = jnp.zeros_like(cum)
        wide[...] = jnp.zeros_like(wide)
        wide[0:1, 0:head_count] = bias_ref[...]
        wide[1:2, 0:head_count] = rates_ref[...]
        first = (lax.axis_index("col") * pieces + lax.axis_index("row")) * events
        halo = jnp.where(first == 0, -1, halo_ref[0])
        names = jnp.concatenate([halo, ids_ref[0]], axis=1).astype(F32)
        position = first + lax.broadcasted_iota(jnp.int32, (1, events), 1)
        kept = jnp.where(position < lengths_ref[user], masks_ref[0], 0)
        kept = jnp.where(kept > 0, 1.0, 0.0).astype(F32)
        flags = jnp.concatenate([jnp.zeros((1, STRETCH), F32), kept], axis=1)
        line = lax.broadcasted_iota(jnp.int32, (8, STRETCH + events), 0)
        meta = jnp.transpose(jnp.where(line == 0, names, jnp.where(line == 1, flags, 0.0)))
        usebuf[...] = meta[STRETCH:, :]
        ids = meta[STRETCH - HALO :, 0:1].astype(jnp.int32)
        items = tin_ref.shape[0]
        lane = lax.broadcasted_iota(jnp.int32, (HALO + events, items), 1)
        hot = (ids == lane).astype(F32).astype(BF16)
        rowbuf[...] = jnp.dot(hot, tin_ref[...], preferred_element_type=F32)
        now = hot[HALO:]
        gate_ref[...] = jnp.dot(now, tgate_ref[...], preferred_element_type=F32).astype(BF16)
        partbuf[...] = jnp.dot(now, tdt_ref[...], preferred_element_type=F32)

    base = pl.multiple_of(place * STRETCH, STRETCH)
    usable = usebuf[pl.ds(base, STRETCH), :][:, 1:2]
    parts = partbuf[pl.ds(base, STRETCH), :]
    raw = (
        parts
        + pltpu.roll(parts, LANES - head_count, 1)
        + pltpu.roll(parts, LANES - 2 * head_count, 1)
    )
    raw = raw + wide[0:1, :]
    step = usable * (jnp.maximum(raw, 0.0) + jnp.log1p(jnp.exp(-jnp.abs(raw))))
    rows = lax.broadcasted_iota(jnp.int32, (STRETCH, STRETCH), 0)
    cols = lax.broadcasted_iota(jnp.int32, (STRETCH, STRETCH), 1)
    causal = rows >= cols
    logs = jnp.dot(
        jnp.where(causal, 1.0, 0.0).astype(F32),
        step * wide[1:2, :],
        precision=lax.Precision.HIGHEST,
        preferred_element_type=F32,
    )
    total = logs[STRETCH - 1 :, :]
    logs_t = jnp.transpose(logs)
    step_t = jnp.transpose(step)
    kernel = taps_ref.shape[0]
    window = rowbuf[pl.ds(base, HALO + STRETCH), :]
    conv = window * taps_ref[0:1, :]
    for k in range(1, kernel):
        conv = pltpu.roll(conv, 1, 0) + window * taps_ref[k : k + 1, :]
    conv = conv[HALO:, :]
    signal = silu(conv[:, :inner]).astype(BF16)
    inward = conv[:, inner : inner + state_width].astype(BF16)
    outward = conv[:, inner + state_width :].astype(BF16)
    out_ref[...] = outward
    scores = lax.dot_general(
        outward, inward, (((1,), (1,)), ((), ())), preferred_element_type=F32
    )
    scores = jnp.where(causal, scores, 0.0)
    tail = jnp.exp(logs - total) * step
    fade = jnp.exp(-logs)
    held = jnp.dot(outward, run[...].astype(BF16), preferred_element_type=F32)
    for h in range(head_count):
        span = slice(h * head_size, (h + 1) * head_size)
        gap = jnp.minimum(logs_t[h : h + 1, :] - logs[:, h : h + 1], 0.0)
        weights = (jnp.exp(gap) * (scores * step_t[h : h + 1, :])).astype(BF16)
        near = jnp.dot(weights, signal[:, span], preferred_element_type=F32)
        y_ref[:, span] = (near + held[:, span] * fade[:, h : h + 1]).astype(BF16)
        scaled[:, span] = (signal[:, span].astype(F32) * tail[:, h : h + 1]).astype(BF16)
    added = lax.dot_general(
        inward, scaled[...], (((0,), (0,)), ((), ())), preferred_element_type=F32
    )
    shrink = jnp.exp(-total)
    for h in range(head_count):
        span = slice(h * head_size, (h + 1) * head_size)
        run[:, span] = run[:, span] * shrink[:, h : h + 1] + added[:, span]
    before = cum[0:1, :]
    lane = lax.broadcasted_iota(jnp.int32, (STRETCH, LANES), 1)
    ef_ref[...] = jnp.where(lane == LANES - 1, usable, jnp.exp(-(logs + before)))
    after = before + total
    cum[...] = jnp.broadcast_to(after, cum.shape)

    @pl.when(place == stretch_count - 1)
    def _():
        width = inner // pieces
        for q in range(pieces):
            state_ref[q, 0] = run[:, q * width : (q + 1) * width].astype(BF16)
            for j in range(width // head_size):
                h = q * (width // head_size) + j
                log_ref[q, 0, :, j * head_size : (j + 1) * head_size] = jnp.broadcast_to(
                    after[:, h : h + 1], (8, head_size)
                )


def chain_kernel(
    rows,
    cols,
    state_ref,
    log_ref,
    enter_ref,
    rin,
    lin,
    before,
    fades,
    pin,
    psend,
    esend,
    s1,
    r1,
    sl,
    rl,
    s2,
    r2,
    s3,
    r3,
):
    users = state_ref.shape[1]
    r, c = lax.axis_index("row"), lax.axis_index("col")
    barrier = pltpu.get_barrier_semaphore()
    for d in range(1, rows):
        pl.semaphore_signal(
            barrier, inc=1, device_id={"row": lax.rem(r + d, rows)}, device_id_type=MESH
        )

    @pl.when(c > 0)
    def _():
        pl.semaphore_signal(barrier, inc=1, device_id={"col": c - 1}, device_id_type=MESH)

    @pl.when(c < cols - 1)
    def _():
        pl.semaphore_signal(barrier, inc=1, device_id={"col": c + 1}, device_id_type=MESH)

    peers = rows - 1 + jnp.where(c > 0, 1, 0) + jnp.where(c < cols - 1, 1, 0)
    pl.semaphore_wait(barrier, peers)

    first = [[] for _ in range(users)]
    for u in range(users):
        for d in range(1, rows):
            q = lax.rem(r + d, rows)
            for source, target, send, recv in (
                (log_ref, lin, sl, rl),
                (state_ref, rin, s1, r1),
            ):
                copy = pltpu.make_async_remote_copy(
                    src_ref=source.at[q, u],
                    dst_ref=target.at[r, u],
                    send_sem=send.at[d, u],
                    recv_sem=recv.at[d, u],
                    device_id={"row": q},
                    device_id_type=MESH,
                )
                copy.start()
                first[u].append(copy)
    rin[r] = state_ref[r]
    lin[r] = log_ref[r]
    onward = [
        pltpu.make_async_remote_copy(
            src_ref=psend.at[u],
            dst_ref=pin.at[u],
            send_sem=s2.at[u],
            recv_sem=r2.at[u],
            device_id={"col": lax.rem(c + 1, cols)},
            device_id_type=MESH,
        )
        for u in range(users)
    ]

    for u in range(users):
        for copy in first[u]:
            copy.wait_recv()
        carried = jnp.zeros(pin.shape[1:], F32)
        fade = jnp.ones((1, pin.shape[2]), F32)
        for m in range(rows):
            before[m, u] = carried
            fades[m, u] = jnp.broadcast_to(fade, fades.shape[2:])
            here = jnp.exp(-lin[m, u, 0:1, :])
            carried = here * carried + rin[m, u].astype(F32)
            fade = fade * here
        before[rows, u] = carried
        fades[rows, u] = jnp.broadcast_to(fade, fades.shape[2:])
        if cols > 1:

            @pl.when(c == 0)
            def _(u=u, carried=carried):
                psend[u] = carried.astype(BF16)
                onward[u].start()

    @pl.when(c == 0)
    def _():
        pin[...] = jnp.zeros_like(pin)

    third = []
    for u in range(users):

        @pl.when(c > 0)
        def _(u=u):
            onward[u].wait_recv()

        @pl.when(jnp.logical_and(c > 0, c < cols - 1))
        def _(u=u):
            psend[u] = (fades[rows, u, 0:1, :] * pin[u].astype(F32) + before[rows, u]).astype(BF16)
            onward[u].start()

        for d in range(1, rows):
            q = lax.rem(r + d, rows)
            esend[d, u] = (fades[q, u, 0:1, :] * pin[u].astype(F32) + before[q, u]).astype(BF16)
            copy = pltpu.make_async_remote_copy(
                src_ref=esend.at[d, u],
                dst_ref=enter_ref.at[r, u],
                send_sem=s3.at[d, u],
                recv_sem=r3.at[d, u],
                device_id={"row": q},
                device_id_type=MESH,
            )
            copy.start()
            third.append(copy)
        enter_ref[r, u] = (fades[r, u, 0:1, :] * pin[u].astype(F32) + before[r, u]).astype(BF16)
    for copy in third:
        copy.wait()
    for group in first:
        for copy in group:
            copy.wait_send()

    @pl.when(c < cols - 1)
    def _():
        for copy in onward:
            copy.wait_send()


def finish_kernel(
    head_count, y_ref, gate_ref, outward_ref, ef_ref, enter_ref, gain_ref, wout_ref, result_ref, mix
):
    pieces, _, _, width = enter_ref.shape
    inner = pieces * width
    head_size = inner // head_count
    squares = None
    for q in range(pieces):
        far = jnp.dot(outward_ref[...], enter_ref[q, 0], preferred_element_type=F32)
        for j in range(width // head_size):
            h = q * (width // head_size) + j
            span = slice(h * head_size, (h + 1) * head_size)
            both = y_ref[:, span].astype(F32) + far[:, j * head_size : (j + 1) * head_size] * ef_ref[:, h : h + 1]
            value = both * silu(gate_ref[:, span].astype(F32))
            mix[:, span] = value
            squares = value * value if squares is None else squares + value * value
    mean = jnp.sum(squares, axis=1, keepdims=True) * (1.0 / inner)
    normed = (mix[...] * lax.rsqrt(mean + 1.0) * gain_ref[...]).astype(BF16)
    result = jnp.dot(normed, wout_ref[...], preferred_element_type=F32)
    result_ref[...] = (result * ef_ref[:, LANES - 1 : LANES]).astype(BF16)


def per_device(
    item_ids,
    pad_masks,
    lengths,
    item_table,
    w_gate,
    w_in,
    w_dt,
    conv_taps,
    dt_bias,
    decay_rates,
    norm_gain,
    w_out,
):
    users = item_ids.shape[0]
    events = item_ids.shape[2]
    items, model = item_table.shape
    full_width = w_in.shape[1]
    inner = w_gate.shape[1]
    head_count = decay_rates.shape[0]
    head_size = inner // head_count
    state_width = (full_width - inner) // 2
    rows, cols = lax.axis_size("row"), lax.axis_size("col")
    stretch_count = events // STRETCH
    steps = users * stretch_count
    width = inner // rows

    def whole(shape):
        return pl.BlockSpec(shape, lambda s: (0,) * len(shape))

    def by_rows(columns):
        return pl.BlockSpec((STRETCH, columns), lambda s: (s, 0))

    total_rows = users * events
    block = 2 * LANES
    in_blocks, gate_blocks = full_width // block, inner // block
    table_in, table_gate, table_dt, halo = pl.pallas_call(
        functools.partial(project_kernel, (in_blocks, gate_blocks, head_count), (rows, cols)),
        grid=(max(in_blocks, gate_blocks),),
        in_specs=[
            whole(item_ids.shape),
            whole((items, model)),
            pl.BlockSpec((model, block), lambda s: (0, jnp.minimum(s, in_blocks - 1))),
            pl.BlockSpec((model, block), lambda s: (0, jnp.minimum(s, gate_blocks - 1))),
            whole(w_dt.shape[::-1]),
        ],
        out_specs=[
            pl.BlockSpec((items, block), lambda s: (0, jnp.minimum(s, in_blocks - 1))),
            pl.BlockSpec((items, block), lambda s: (0, jnp.minimum(s, gate_blocks - 1))),
            whole((items, LANES)),
            whole((users, 1, STRETCH)),
        ],
        out_shape=[
            jax.ShapeDtypeStruct((items, full_width), BF16),
            jax.ShapeDtypeStruct((items, inner), BF16),
            jax.ShapeDtypeStruct((items, LANES), BF16),
            jax.ShapeDtypeStruct((users, 1, STRETCH), jnp.int32),
        ],
        scratch_shapes=[
            pltpu.VMEM((LANES, model), BF16),
            pltpu.VMEM((users, 1, STRETCH), jnp.int32),
            pltpu.SemaphoreType.DMA,
            pltpu.SemaphoreType.DMA,
        ],
        compiler_params=pltpu.CompilerParams(
            dimension_semantics=("arbitrary",), collective_id=1, has_side_effects=True
        ),
        cost_estimate=pl.CostEstimate(
            flops=2 * items * model * (full_width + inner),
            bytes_accessed=4 * model * (full_width + inner),
            transcendentals=0,
        ),
        name="table_part",
    )(item_ids, item_table, w_in, w_gate, w_dt.T)

    def by_user(columns):
        return pl.BlockSpec((1, 1, columns), lambda s: (s // stretch_count, 0, 0))

    y, gate, outward, ef, state, logs = pl.pallas_call(
        functools.partial(
            local_kernel, (stretch_count, head_count, head_size, state_width, rows)
        ),
        grid=(steps,),
        in_specs=[
            pl.BlockSpec(memory_space=pltpu.SMEM),
            by_user(events),
            by_user(STRETCH),
            by_user(events),
            whole((items, full_width)),
            whole((items, inner)),
            whole((items, LANES)),
            whole(conv_taps.shape),
            whole((1, head_count)),
            whole((1, head_count)),
        ],
        out_specs=[
            by_rows(inner),
            pl.BlockSpec((events, inner), lambda s: (s // stretch_count, 0)),
            by_rows(state_width),
            by_rows(LANES),
            pl.BlockSpec((rows, 1, state_width, width), lambda s: (0, s // stretch_count, 0, 0)),
            pl.BlockSpec((rows, 1, 8, width), lambda s: (0, s // stretch_count, 0, 0)),
        ],
        out_shape=[
            jax.ShapeDtypeStruct((total_rows, inner), BF16),
            jax.ShapeDtypeStruct((total_rows, inner), BF16),
            jax.ShapeDtypeStruct((total_rows, state_width), BF16),
            jax.ShapeDtypeStruct((total_rows, LANES), F32),
            jax.ShapeDtypeStruct((rows, users, state_width, width), BF16),
            jax.ShapeDtypeStruct((rows, users, 8, width), F32),
        ],
        scratch_shapes=[
            pltpu.VMEM((HALO + events, full_width), F32),
            pltpu.VMEM((events, LANES), F32),
            pltpu.VMEM((events, 8), F32),
            pltpu.VMEM((8, LANES), F32),
            pltpu.VMEM((STRETCH, inner), BF16),
            pltpu.VMEM((state_width, inner), F32),
            pltpu.VMEM((8, LANES), F32),
        ],
        compiler_params=pltpu.CompilerParams(dimension_semantics=("arbitrary",)),
        name="local_part",
    )(
        lengths,
        item_ids,
        halo,
        pad_masks,
        table_in,
        table_gate,
        table_dt,
        conv_taps,
        dt_bias[None],
        decay_rates[None],
    )

    vmem = pl.BlockSpec(memory_space=pltpu.VMEM)
    dma = pltpu.SemaphoreType.DMA
    entering = pl.pallas_call(
        functools.partial(chain_kernel, rows, cols),
        in_specs=[vmem, vmem],
        out_specs=vmem,
        out_shape=jax.ShapeDtypeStruct(state.shape, BF16),
        scratch_shapes=[
            pltpu.VMEM(state.shape, BF16),
            pltpu.VMEM(logs.shape, F32),
            pltpu.VMEM((rows + 1,) + state.shape[1:], F32),
            pltpu.VMEM((rows + 1,) + logs.shape[1:], F32),
            pltpu.VMEM(state.shape[1:], BF16),
            pltpu.VMEM(state.shape[1:], BF16),
            pltpu.VMEM(state.shape, BF16),
            dma((rows, users)),
            dma((rows, users)),
            dma((rows, users)),
            dma((rows, users)),
            dma((users,)),
            dma((users,)),
            dma((rows, users)),
            dma((rows, users)),
        ],
        compiler_params=pltpu.CompilerParams(collective_id=0, has_side_effects=True),
        name="state_chain",
    )(state, logs)

    tall = 2 * STRETCH if events % (2 * STRETCH) == 0 else STRETCH

    def tall_rows(columns):
        return pl.BlockSpec((tall, columns), lambda s: (s, 0))

    result = pl.pallas_call(
        functools.partial(finish_kernel, head_count),
        grid=(total_rows // tall,),
        in_specs=[
            tall_rows(inner),
            tall_rows(inner),
            tall_rows(state_width),
            tall_rows(LANES),
            pl.BlockSpec((rows, 1, state_width, width), lambda s: (0, s // (events // tall), 0, 0)),
            whole((1, inner)),
            whole(w_out.shape),
        ],
        out_specs=tall_rows(w_out.shape[1]),
        out_shape=jax.ShapeDtypeStruct((total_rows, w_out.shape[1]), BF16),
        scratch_shapes=[pltpu.VMEM((tall, inner), F32)],
        compiler_params=pltpu.CompilerParams(dimension_semantics=("arbitrary",)),
        name="finish_part",
    )(y, gate, outward, ef, entering, norm_gain[None], w_out)
    return result.reshape(users, 1, events, -1)


def solution(mesh):
    in_specs = (
        P("batch", "col", "row"),
        P("batch", "col", "row"),
        P("batch"),
        P(),
        P(),
        P(),
        P(),
        P(),
        P(),
        P(),
        P(),
        P(),
    )
    out_specs = P("batch", "col", "row", None)
    return jax.shard_map(
        per_device, mesh=mesh, in_specs=in_specs, out_specs=out_specs, check_vma=False
    )
```
